256 devices in a mesh: dom: 8 (over y, core), mem: 32 (over z, x).
Axes of the slice: x: 4, y: 4, z: 8, core: 2. Of those that a mesh axis runs over, the one named last changes fastest.
Arguments:
- control: bfloat16 [256, 128, 16384], P('mem', None, 'dom'), may hold values from -6 to 6
- corr_offsets: int32 [128, 4], P('dom'), may hold values from -2 to 2, as said below
- corr_blocks: bfloat16 [128, 4, 128, 128], P('dom'), may hold values from -0.25 to 0.25
- interp_index: int32 [128, 4], P('dom'), may hold values from 0 to 15
- interp_blocks: bfloat16 [128, 4, 128, 128], P('dom'), may hold values from -0.25 to 0.25
- perturbations: bfloat16 [256, 128, 16384], P('mem', None, 'dom'), may hold values from -6 to 6
Outputs:
- increment: bfloat16 [128, 16384], P(None, 'dom')
The draws below stay inside these ranges and needn't reach their ends.
Inputs may be any that keep to these rules, and one draw needn't show every extreme that they name: `corr_offsets`: each row holds 4 distinct offsets, among them 0, -2 and 2; exactly one of -1 and 1 is absent from each row. `interp_index`: an entry names a subgrid block of the tile that owns the column block, counted from that tile's first block.
All inputs are finite; a program needn't handle non-finite values.
Results may differ from the reference program's by a relative error of at most 0.0049.
Values may be sent and summed in bfloat16 or wider, within the bound.
No kernel may reach another device: no remote copies, remote signals or barrier semaphores. Data moves between devices by JAX's collectives and lax.ppermute only.
A program may use at most 128 MiB of HBM per device.

```python
import jax
import jax.numpy as jnp
import numpy as np
from jax import lax

BLK = 128
HR = 2
NI = 4
LEV = 128
SB_DEV = 16
COLB_DEV = 16
NNZ = 4
MEMBERS = 256
NBLK = 128
SUB = 16384
NCOLB = 128
COLS = 16384


def draw_corr_offsets(key, part):
    without_low = np.array([shift for shift in range(-HR, HR + 1) if shift != -1], np.int32)
    without_high = np.array([shift for shift in range(-HR, HR + 1) if shift != 1], np.int32)
    first_key, second_key = jax.random.split(jax.random.fold_in(key, 11))
    choose = jax.random.randint(first_key, (NBLK, 1), 0, 2)
    kept = jnp.where(choose == 0, jnp.asarray(without_low)[None, :], jnp.asarray(without_high)[None, :])
    scores = jax.random.randint(second_key, (NBLK, NNZ), 0, 1 << 20) * NNZ + jnp.arange(NNZ, dtype=jnp.int32)[None, :]
    arrangement = jnp.argsort(scores, axis=1)
    return jnp.take_along_axis(kept, arrangement, axis=1).astype(jnp.int32)


def set_ends(values, rng, smallest, high):
    index_at = [jax.random.randint(jax.random.fold_in(rng, axis), (), 0, length) for axis, length in enumerate(values.shape)]
    widest = values.shape.index(max(values.shape))
    neighbour = index_at[:widest] + [(index_at[widest] + 1) % values.shape[widest]] + index_at[widest + 1:]
    return values.at[tuple(index_at)].set(smallest).at[tuple(neighbour)].set(high)


def with_spikes(values, stream_key, source, target, shards_of, factor):
    owner, partner = [(jnp.arange(values.shape[dim]) // (values.shape[dim] // shards_of)).reshape([-1 if axis == dim else 1 for axis in range(values.ndim)]) for dim in (source, target)]
    chosen = jax.random.permutation(stream_key, shards_of)[partner]
    strong = (owner == chosen) | (owner == (partner + shards_of // 2) % shards_of)
    return jnp.where(strong, factor * values, values)


def steps_of(own_key, shape, shards, low, largest):
    def one(dim, blocks):
        steps = jax.random.uniform(jax.random.fold_in(jax.random.fold_in(own_key, 6), dim), (blocks,), jnp.float32, low / len(shards), largest / len(shards))
        return jnp.repeat(jnp.exp(steps), shape[dim] // blocks).reshape((-1,) + (1,) * (len(shape) - dim - 1))

    loudness = one(*shards[0])
    for cut in shards[1:]:
        loudness = loudness * one(*cut)
    return loudness


def bell_draw(rng, extent, scale, limit, pieces=(), kind=jnp.bfloat16):
    entries = jax.random.normal(rng, extent, jnp.float32) * scale
    if len(pieces) > 0:
        entries = steps_of(rng, extent, pieces, -0.22, 0.18) * entries
    return jnp.clip(entries, min=-limit, max=limit).astype(kind)


def gaussian_with(stream_key, dims, deviation, bound, shards, heavy, kind=jnp.bfloat16):
    result = deviation * jax.random.normal(stream_key, dims, jnp.float32)
    if shards:
        result = result * steps_of(stream_key, dims, shards, -0.22, 0.18)
    return jnp.clip(with_spikes(result, jax.random.fold_in(stream_key, 3), *heavy), -bound, bound).astype(kind)


def setup_inputs(seed: int = 0) -> dict:
    streams_of = jax.random.split(jax.random.key(seed), 7)
    return {
        "control": bell_draw(streams_of[0], (MEMBERS, LEV, SUB), 1.0, 6.0, ((0, 32), (2, 8))),
        "corr_offsets": draw_corr_offsets(jax.random.fold_in(streams_of[6], 71), 0),
        "corr_blocks": bell_draw(streams_of[2], (NBLK, NNZ, BLK, BLK), (NNZ * BLK) ** -0.5, 0.25, ((0, 8),)),
        "interp_index": set_ends(jax.random.randint(streams_of[3], (NCOLB, NI), 0, SB_DEV), jax.random.fold_in(streams_of[3], 1), 0, SB_DEV - 1).astype(jnp.int32),
        "interp_blocks": bell_draw(streams_of[4], (NCOLB, NI, BLK, BLK), (NI * BLK) ** -0.5, 0.25, ((0, 8),)),
        "perturbations": gaussian_with(streams_of[5], (MEMBERS, LEV, COLS), 1.0, 6.0, ((0, 32), (2, 8)), (0, 1, 32, 2.75)),
    }


def reference(control, corr_offsets, corr_blocks, interp_index, interp_blocks, perturbations):
    blocks_all = corr_blocks.shape[0]
    breadth = corr_blocks.shape[2]
    column_blocks = interp_blocks.shape[0]
    levels = control.shape[1]
    source = (jnp.arange(blocks_all, dtype=jnp.int32)[:, None] + corr_offsets.astype(jnp.int32)) % blocks_all
    owner_tile = jnp.arange(column_blocks, dtype=jnp.int32) // COLB_DEV
    feeding = owner_tile[:, None] * SB_DEV + interp_index.astype(jnp.int32)
    corr_wide = corr_blocks.astype(jnp.float32)
    interp_wide = interp_blocks.astype(jnp.float32)

    def one_member(summed, paired):
        member_control, member_pert = paired
        tiled = member_control.astype(jnp.float32).reshape(levels, blocks_all, breadth)
        smoothed = jnp.einsum('lbsj,bsji->lbi', tiled[:, source], corr_wide, precision=lax.Precision.HIGHEST)
        smoothed = smoothed.astype(jnp.bfloat16).astype(jnp.float32)
        spread = jnp.einsum('lqkj,qkji->lqi', smoothed[:, feeding], interp_wide, precision=lax.Precision.HIGHEST)
        updated = summed + member_pert.astype(jnp.float32) * spread.reshape(levels, column_blocks * breadth)
        return (updated, None)
    initial = jnp.zeros((levels, column_blocks * breadth), jnp.float32)
    summed = lax.scan(one_member, initial, (control, perturbations))[0]
    factor = 1.0 / jnp.sqrt(jnp.float32(MEMBERS - 1))
    return (summed * factor).astype(jnp.bfloat16)
```

```python
import jax
import jax.numpy as jnp
from jax import lax
from jax.experimental import pallas as pl
from jax.experimental.pallas import tpu as pltpu
from jax.sharding import PartitionSpec as P

HR = 2
ANY = pl.BlockSpec(memory_space=pl.ANY)
SMEM = pl.BlockSpec(memory_space=pltpu.SMEM)
VMEM = pl.BlockSpec(memory_space=pltpu.VMEM)


def ring_halos(control, width):
    count = lax.axis_size("dom")
    forward = [(i, (i + 1) % count) for i in range(count)]
    backward = [(target, source) for source, target in forward]
    low = lax.ppermute(control[:, -width:], "dom", forward)
    high = lax.ppermute(control[:, :width], "dom", backward)
    return low, high


def smooth_inner(control, corr_offsets, corr_blocks):
    rows, width = control.shape
    blocks, stored, breadth = corr_blocks.shape[:3]
    inner = blocks - 2 * HR
    depth = stored * breadth
    pair = 2 * breadth

    def kernel(offsets, control_hbm, corr_hbm, out_hbm, tile, corr, out, tile_sem, corr_sem, out_sem):
        def tile_copy(c):
            return pltpu.make_async_copy(
                control_hbm.at[:, pl.ds(c * pair, pair)],
                tile.at[:, pl.ds(c * pair, pair)],
                tile_sem.at[c],
            )

        def corr_copy(c):
            return pltpu.make_async_copy(
                corr_hbm.at[pl.ds(HR + 2 * c, 2)], corr.at[pl.ds(2 * c, 2)], corr_sem.at[c]
            )

        for c in range(4):
            tile_copy(c).start()
        for c in range(2):
            corr_copy(c).start()
        tile_copy(0).wait()
        tile_copy(1).wait()
        for c in range(inner // 2):
            tile_copy(c + 2).wait()
            corr_copy(c).wait()
            if c + 4 < blocks // 2:
                tile_copy(c + 4).start()
            if c + 2 < inner // 2:
                corr_copy(c + 2).start()
            for i in (2 * c, 2 * c + 1):
                sources = [
                    tile[:, pl.ds(pl.multiple_of((HR + i + offsets[s, HR + i]) * breadth, breadth), breadth)]
                    for s in range(stored)
                ]
                result = jnp.dot(
                    jnp.concatenate(sources, axis=1),
                    corr[i].reshape(depth, breadth),
                    preferred_element_type=jnp.float32,
                )
                out[i] = result.astype(jnp.bfloat16)
            pltpu.make_async_copy(
                out.at[pl.ds(2 * c, 2)], out_hbm.at[pl.ds(2 * c, 2)], out_sem.at[c]
            ).start()
        for c in range(inner // 2):
            pltpu.make_async_copy(
                out.at[pl.ds(2 * c, 2)], out_hbm.at[pl.ds(2 * c, 2)], out_sem.at[c]
            ).wait()

    return pl.pallas_call(
        kernel,
        out_shape=jax.ShapeDtypeStruct((inner, rows, breadth), jnp.bfloat16),
        in_specs=[SMEM, ANY, ANY],
        out_specs=ANY,
        scratch_shapes=[
            pltpu.VMEM((rows, width), jnp.bfloat16),
            pltpu.VMEM((inner, stored, breadth, breadth), jnp.bfloat16),
            pltpu.VMEM((inner, rows, breadth), jnp.bfloat16),
            pltpu.SemaphoreType.DMA((blocks // 2,)),
            pltpu.SemaphoreType.DMA((inner // 2,)),
            pltpu.SemaphoreType.DMA((inner // 2,)),
        ],
        compiler_params=pltpu.CompilerParams(vmem_limit_bytes=60 * 1024 * 1024),
        cost_estimate=pl.CostEstimate(
            flops=2 * rows * depth * breadth * inner,
            bytes_accessed=2 * rows * (width + inner * breadth),
            transcendentals=0,
        ),
        name="smooth_inner",
    )(corr_offsets.T, control, corr_blocks)


def member_sums(
    control, low, high, inner_smoothed, corr_offsets, corr_blocks, interp_index, interp_blocks,
    perturbations, members, xs,
):
    rows, width = control.shape
    blocks, stored, breadth = corr_blocks.shape[:3]
    column_blocks, feeding = interp_blocks.shape[:2]
    levels = rows // members
    part = levels // xs
    halo = HR * breadth
    inner = blocks - 2 * HR
    pair = 2 * breadth

    def kernel(
        offsets, index, control_hbm, low_hbm, high_hbm, inner_hbm, corr_hbm, interp_hbm, pert_hbm,
        out, left, right, corr, smoothed, interp, pert, edge_sem, inner_sem, interp_sem, pert_sem,
    ):
        edge = [
            pltpu.make_async_copy(low_hbm, left.at[:, pl.ds(0, halo)], edge_sem.at[0]),
            pltpu.make_async_copy(
                control_hbm.at[:, pl.ds(0, 2 * halo)], left.at[:, pl.ds(halo, 2 * halo)], edge_sem.at[1]
            ),
            pltpu.make_async_copy(corr_hbm.at[pl.ds(0, HR)], corr.at[pl.ds(0, HR)], edge_sem.at[2]),
            pltpu.make_async_copy(
                control_hbm.at[:, pl.ds(width - 2 * halo, 2 * halo)],
                right.at[:, pl.ds(0, 2 * halo)],
                edge_sem.at[3],
            ),
            pltpu.make_async_copy(high_hbm, right.at[:, pl.ds(2 * halo, halo)], edge_sem.at[4]),
            pltpu.make_async_copy(
                corr_hbm.at[pl.ds(blocks - HR, HR)], corr.at[pl.ds(HR, HR)], edge_sem.at[5]
            ),
        ]
        inner_copy = pltpu.make_async_copy(inner_hbm, smoothed.at[pl.ds(HR, inner)], inner_sem)

        def column_copies(c):
            return (
                pltpu.make_async_copy(
                    interp_hbm.at[pl.ds(2 * c, 2)], interp.at[pl.ds(2 * c, 2)], interp_sem.at[c]
                ),
                pltpu.make_async_copy(
                    pert_hbm.at[:, pl.ds(c * pair, pair)],
                    pert.at[:, pl.ds(c * pair, pair)],
                    pert_sem.at[c],
                ),
            )

        for copy in edge:
            copy.start()
        for side in range(2):
            for copy in edge[3 * side : 3 * side + 3]:
                copy.wait()
            if side == 0:
                inner_copy.start()
            for copy in column_copies(side):
                copy.start()
            span = right if side else left
            for i in range(HR):
                b = blocks - HR + i if side else i
                first = blocks - 2 * HR if side else -HR
                sources = [
                    span[:, pl.ds(pl.multiple_of((b - first + offsets[s, b]) * breadth, breadth), breadth)]
                    for s in range(stored)
                ]
                result = jnp.dot(
                    jnp.concatenate(sources, axis=1),
                    corr[side * HR + i].reshape(stored * breadth, breadth),
                    preferred_element_type=jnp.float32,
                )
                smoothed[b] = result.astype(jnp.bfloat16)
        inner_copy.wait()
        for c in range(column_blocks // 2):
            for copy in column_copies(c):
                copy.wait()
            if c + 2 < column_blocks // 2:
                for copy in column_copies(c + 2):
                    copy.start()
            for i in range(2):
                q = 2 * c + i
                lhs = jnp.concatenate([smoothed[index[k, q]] for k in range(feeding)], axis=1)
                spread = jnp.dot(
                    lhs, interp[q].reshape(feeding * breadth, breadth), preferred_element_type=jnp.float32
                )
                term = pert[:, pl.ds(q * breadth, breadth)].astype(jnp.float32) * spread
                total = jnp.sum(term.reshape(members, levels, breadth), axis=0).astype(jnp.bfloat16)
                for x in range(xs):
                    out[c * xs + x, :, i * breadth : (i + 1) * breadth] = total[x * part : (x + 1) * part]

    return pl.pallas_call(
        kernel,
        out_shape=jax.ShapeDtypeStruct((column_blocks // 2 * xs, part, pair), jnp.bfloat16),
        in_specs=[SMEM, SMEM] + [ANY] * 7,
        out_specs=VMEM,
        scratch_shapes=[
            pltpu.VMEM((rows, 3 * halo), jnp.bfloat16),
            pltpu.VMEM((rows, 3 * halo), jnp.bfloat16),
            pltpu.VMEM((2 * HR, stored, breadth, breadth), jnp.bfloat16),
            pltpu.VMEM((blocks, rows, breadth), jnp.bfloat16),
            pltpu.VMEM((column_blocks, feeding, breadth, breadth), jnp.bfloat16),
            pltpu.VMEM((rows, width), jnp.bfloat16),
            pltpu.SemaphoreType.DMA((6,)),
            pltpu.SemaphoreType.DMA,
            pltpu.SemaphoreType.DMA((column_blocks // 2,)),
            pltpu.SemaphoreType.DMA((column_blocks // 2,)),
        ],
        compiler_params=pltpu.CompilerParams(vmem_limit_bytes=60 * 1024 * 1024),
        cost_estimate=pl.CostEstimate(
            flops=2 * rows * feeding * breadth * breadth * (column_blocks + 2 * HR),
            bytes_accessed=6 * rows * width,
            transcendentals=0,
        ),
        name="member_sums",
    )(
        corr_offsets.T, interp_index.T, control, low, high, inner_smoothed, corr_blocks,
        interp_blocks, perturbations,
    )


def sum_received(parts, factor, repeats):
    def kernel(parts_ref, out_ref):
        total = jnp.sum(parts_ref[...].astype(jnp.float32), axis=0) * factor
        out_ref[...] = jnp.broadcast_to(total.astype(jnp.bfloat16)[None], out_ref.shape)

    return pl.pallas_call(
        kernel,
        out_shape=jax.ShapeDtypeStruct((repeats,) + parts.shape[1:], jnp.bfloat16),
        in_specs=[VMEM],
        out_specs=VMEM,
        compiler_params=pltpu.CompilerParams(vmem_limit_bytes=8 * 1024 * 1024),
        name="sum_received",
    )(parts)


def assemble(position, pieces):
    xs = len(pieces)
    zs, part, pair = pieces[0].shape

    def kernel(position_ref, *refs):
        out = refs[-1]
        for k in range(xs):
            x = lax.rem(position_ref[0] + xs - k, xs)
            rows = pl.ds(pl.multiple_of(x * part, part), part)
            for z in range(zs):
                out[rows, z * pair : (z + 1) * pair] = refs[k][z]

    return pl.pallas_call(
        kernel,
        out_shape=jax.ShapeDtypeStruct((xs * part, zs * pair), jnp.bfloat16),
        in_specs=[SMEM] + [VMEM] * xs,
        out_specs=VMEM,
        compiler_params=pltpu.CompilerParams(vmem_limit_bytes=8 * 1024 * 1024),
        name="assemble",
    )(position, *pieces)


def per_device(control, corr_offsets, corr_blocks, interp_index, interp_blocks, perturbations):
    members, levels, width = control.shape
    breadth = corr_blocks.shape[2]
    xs = lax.axis_size("x")
    zs = lax.axis_size("z")
    members_all = members * zs * xs
    factor = float(1.0 / (members_all - 1) ** 0.5)
    rows = control.reshape(members * levels, width)
    low, high = ring_halos(rows, HR * breadth)
    inner = smooth_inner(rows, corr_offsets, corr_blocks)
    sums = member_sums(
        rows, low, high, inner, corr_offsets, corr_blocks, interp_index, interp_blocks,
        perturbations.reshape(members * levels, width), members, xs,
    )
    parts = lax.all_to_all(sums, ("z", "x"), 0, 0)
    share = sum_received(parts, factor, zs)
    column = lax.all_to_all(share, "z", 0, 0)
    pieces = [column]
    for k in range(1, xs):
        pieces.append(lax.ppermute(column, "x", [(i, (i + k) % xs) for i in range(xs)]))
    position = lax.axis_index("x").astype(jnp.int32).reshape(1)
    return assemble(position, pieces)


def solution(mesh):
    zs = 8
    xs = mesh.shape["mem"] // zs
    inner_mesh = jax.sharding.Mesh(
        mesh.devices.reshape(mesh.shape["dom"], zs, xs), ("dom", "z", "x")
    )
    mem = ("z", "x")
    in_specs = (
        P(mem, None, "dom"),
        P("dom", None),
        P("dom", None, None, None),
        P("dom", None),
        P("dom", None, None, None),
        P(mem, None, "dom"),
    )
    out_specs = P(None, "dom")
    return jax.shard_map(
        per_device, mesh=inner_mesh, in_specs=in_specs, out_specs=out_specs, check_vma=False
    )
```

```python
import jax
import jax.numpy as jnp
from jax import lax
from jax.experimental import pallas as pl
from jax.experimental.pallas import tpu as pltpu
from jax.sharding import PartitionSpec as P

HR = 2
GROUPS = ((2,), (1,), (3,), (0,))
STAGES = (2, 6)
K1_LIMIT = 24
K2_LIMIT = 24
HBM = pl.BlockSpec(memory_space=pltpu.HBM)
VMEM = pl.BlockSpec(memory_space=pltpu.VMEM)


def in_hbm(array):
    return pltpu.with_memory_space_constraint(array, pltpu.HBM)


def tile_halos(rows, width):
    span = rows.shape[1] - width

    def kernel(rows_hbm, first, second, sem):
        odd = lax.rem(lax.axis_index("dom"), 2)
        copies = [
            pltpu.make_async_copy(
                rows_hbm.at[:, pl.ds(pl.multiple_of(part * span, width), width)], out, sem.at[i]
            )
            for i, (part, out) in enumerate(((odd, first), (1 - odd, second)))
        ]
        for copy in copies:
            copy.start()
        for copy in copies:
            copy.wait()

    edge = jax.ShapeDtypeStruct((rows.shape[0], width), rows.dtype)
    first, second = pl.pallas_call(
        kernel,
        out_shape=(edge, edge),
        in_specs=[HBM],
        out_specs=(VMEM, VMEM),
        scratch_shapes=[pltpu.SemaphoreType.DMA((2,))],
        compiler_params=pltpu.CompilerParams(vmem_limit_bytes=8 * 1024 * 1024),
        name="tile_edges",
    )(in_hbm(rows))
    count = lax.axis_size("dom")
    above = [(i, (i + 1 if i % 2 else i - 1) % count) for i in range(count)]
    within = [(i, i - 1 if i % 2 else i + 1) for i in range(count)]
    return lax.ppermute(first, "dom", above), lax.ppermute(second, "dom", within)


def smooth_own(control, corr_offsets, corr_blocks, interp_blocks, perturbations):
    rows, width = control.shape
    blocks, stored, breadth = corr_blocks.shape[:3]
    pairs = blocks // 2
    pair = 2 * breadth
    span = 2 + 2 * HR
    halo = HR * breadth

    def kernel(
        offsets_hbm, control_hbm, corr_hbm, interp_hbm, pert_hbm, out, outer, halo_corr, interp,
        pert, offsets, tile, corr, offsets_sem, tile_sem, corr_sem, later_sem,
    ):
        def tile_copy(c):
            return pltpu.make_async_copy(
                control_hbm.at[:, pl.ds(c * pair, pair)],
                tile.at[:, pl.ds(c * pair, pair)],
                tile_sem.at[c],
            )

        def corr_copies(c):
            copies = []
            for j in range(2):
                b = 2 * c + j
                for s in range(stored):
                    row = pl.multiple_of((offsets[s, b] + HR + j) * breadth, breadth)
                    copies.append(
                        pltpu.make_async_copy(
                            corr_hbm.at[b, s],
                            corr.at[c, pl.ds(row, breadth), pl.ds(j * breadth, breadth)],
                            corr_sem.at[c, j * stored + s],
                        )
                    )
            return copies

        def clear(c):
            zero = jnp.zeros((breadth, breadth), corr.dtype)
            for j in range(2):
                absent = HR + j
                for s in range(stored):
                    absent = absent - offsets[s, 2 * c + j]
                columns = pl.ds(j * breadth, breadth)
                corr[c, pl.ds(pl.multiple_of(absent * breadth, breadth), breadth), columns] = zero
                far = (1 - j) * (span - 1)
                corr[c, far * breadth : (far + 1) * breadth, columns] = zero

        def later_copies(g):
            share = rows // len(stages)
            some = pl.ds(g * share, share)
            count = interp_hbm.shape[0] // len(stages)
            blocks_of = pl.ds(g * count, count)
            return (
                pltpu.make_async_copy(pert_hbm.at[some], pert.at[some], later_sem.at[g, 0]),
                pltpu.make_async_copy(
                    interp_hbm.at[blocks_of], interp.at[blocks_of], later_sem.at[g, 1]
                ),
            )

        stages = [range(sum(STAGES[:g]), sum(STAGES[: g + 1])) for g in range(len(STAGES))]
        offsets_copy = pltpu.make_async_copy(offsets_hbm, offsets, offsets_sem)
        offsets_copy.start()
        tile_ends = [min(stage[-1] + 2, pairs) for stage in stages]
        for c in range(tile_ends[0]):
            tile_copy(c).start()
        offsets_copy.wait()

        @pl.loop(0, pairs)
        def _(c):
            for copy in corr_copies(c):
                copy.start()
            clear(c)

            @pl.when(c == stages[0][-1])
            def _():
                for later in range(tile_ends[0], pairs):
                    tile_copy(later).start()

        for g, stage in enumerate(stages):
            for c in range(tile_ends[g - 1] if g else 0, tile_ends[g]):
                tile_copy(c).wait()
            for c in stage:
                for copy in corr_copies(c):
                    copy.wait()
            if g == 0:
                for h in range(len(stages)):
                    for copy in later_copies(h):
                        copy.start()
            for c in stage:
                first = max(2 * c - HR, 0)
                last = min(2 * c + 2 + HR, blocks)
                start = (first - (2 * c - HR)) * breadth
                depth = (last - first) * breadth
                result = jnp.dot(
                    tile[:, first * breadth : last * breadth],
                    corr[c, start : start + depth, :],
                    preferred_element_type=jnp.float32,
                )
                if c == 0 or c == pairs - 1:
                    side = min(c, 1)
                    outer[side] = result
                    low = side * (span * breadth - halo)
                    halo_corr[side] = corr[c, low : low + halo, :]
                else:
                    result = result.astype(jnp.bfloat16)
                    out[2 * c] = result[:, :breadth]
                    out[2 * c + 1] = result[:, breadth:]
        for g in range(len(stages)):
            for copy in later_copies(g):
                copy.wait()

    return pl.pallas_call(
        kernel,
        out_shape=(
            jax.ShapeDtypeStruct((blocks, rows, breadth), jnp.bfloat16),
            jax.ShapeDtypeStruct((2, rows, pair), jnp.float32),
            jax.ShapeDtypeStruct((2, halo, pair), jnp.bfloat16),
            jax.ShapeDtypeStruct(interp_blocks.shape, jnp.bfloat16),
            jax.ShapeDtypeStruct(perturbations.shape, jnp.bfloat16),
        ),
        in_specs=[HBM] * 5,
        out_specs=(VMEM,) * 5,
        scratch_shapes=[
            pltpu.SMEM((stored, blocks), jnp.int32),
            pltpu.VMEM((rows, width), jnp.bfloat16),
            pltpu.VMEM((pairs, span * breadth, pair), jnp.bfloat16),
            pltpu.SemaphoreType.DMA,
            pltpu.SemaphoreType.DMA((pairs,)),
            pltpu.SemaphoreType.DMA((pairs, 2 * stored)),
            pltpu.SemaphoreType.DMA((len(STAGES), 2)),
        ],
        compiler_params=pltpu.CompilerParams(vmem_limit_bytes=K1_LIMIT * 1024 * 1024),
        cost_estimate=pl.CostEstimate(
            flops=2 * rows * stored * breadth * breadth * blocks,
            bytes_accessed=4 * rows * width,
            transcendentals=0,
        ),
        name="smooth_own",
    )(
        in_hbm(corr_offsets.T), in_hbm(control), in_hbm(corr_blocks), in_hbm(interp_blocks),
        in_hbm(perturbations),
    )


def member_sums(smoothed, interp_index, interp_blocks, perturbations, members, xs, distances, halo=None):
    blocks, rows, breadth = smoothed.shape
    column_blocks, feeding = interp_blocks.shape[:2]
    levels = rows // members
    share = column_blocks // xs

    def kernel(index, interp, pert, *refs):
        outs = refs[-len(distances) :]
        position = lax.axis_index("x")
        if halo is None:
            smooth = refs[0]
        else:
            outer_ref, corr, first_ref, second_ref, smooth = refs[1:6]
            odd = lax.rem(lax.axis_index("dom"), 2)
            for side, halo_ref in ((1 - odd, second_ref), (odd, first_ref)):
                result = outer_ref[side] + jnp.dot(
                    halo_ref[...], corr[side], preferred_element_type=jnp.float32
                )
                result = result.astype(jnp.bfloat16)
                b = side * (blocks - HR)
                smooth[b] = result[:, :breadth]
                smooth[b + 1] = result[:, breadth:]
        for distance, out in zip(distances, outs):
            piece = lax.rem(position + distance, xs)
            for i in range(share):
                q = piece * share + i
                lhs = jnp.concatenate([smooth[index[q, k]] for k in range(feeding)], axis=1)
                spread = jnp.dot(
                    lhs,
                    interp[q].reshape(feeding * breadth, breadth),
                    preferred_element_type=jnp.float32,
                )
                columns = pl.ds(pl.multiple_of(q * breadth, breadth), breadth)
                term = pert[:, columns].astype(jnp.float32) * spread
                total = jnp.sum(term.reshape(members, levels, breadth), axis=0)
                out[:, i * breadth : (i + 1) * breadth] = total.astype(jnp.bfloat16)

    pieces = tuple(
        jax.ShapeDtypeStruct((levels, share * breadth), jnp.bfloat16) for _ in distances
    )
    operands = (interp_blocks, perturbations, smoothed) + (halo or ())
    return pl.pallas_call(
        kernel,
        out_shape=pieces if halo is None else (smoothed,) + pieces,
        in_specs=[VMEM] * (1 + len(operands)),
        out_specs=(VMEM,) * (len(pieces) + (halo is not None)),
        input_output_aliases={} if halo is None else {3: 0},
        compiler_params=pltpu.CompilerParams(vmem_limit_bytes=K2_LIMIT * 1024 * 1024),
        cost_estimate=pl.CostEstimate(
            flops=2 * rows * feeding * breadth * breadth * (share * len(distances) + 1),
            bytes_accessed=6 * rows * share * breadth * len(distances),
            transcendentals=0,
        ),
        name="member_sums",
    )(interp_index, *operands)


def sum_pieces(pieces):
    def kernel(*refs):
        total = refs[0][...].astype(jnp.float32)
        for ref in refs[1:-1]:
            total = total + ref[...].astype(jnp.float32)
        refs[-1][...] = total.astype(jnp.bfloat16)

    return pl.pallas_call(
        kernel,
        out_shape=jax.ShapeDtypeStruct(pieces[0].shape, jnp.bfloat16),
        in_specs=[VMEM] * len(pieces),
        out_specs=VMEM,
        compiler_params=pltpu.CompilerParams(vmem_limit_bytes=8 * 1024 * 1024),
        name="sum_pieces",
    )(*pieces)


def sum_received(parts, factor):
    def kernel(parts_ref, out_ref):
        total = jnp.sum(parts_ref[...].astype(jnp.float32), axis=0) * factor
        out_ref[...] = jnp.broadcast_to(total.astype(jnp.bfloat16)[None], out_ref.shape)

    return pl.pallas_call(
        kernel,
        out_shape=jax.ShapeDtypeStruct(parts.shape, jnp.bfloat16),
        in_specs=[VMEM],
        out_specs=VMEM,
        compiler_params=pltpu.CompilerParams(vmem_limit_bytes=8 * 1024 * 1024),
        name="sum_received",
    )(parts)


def assemble(pieces):
    xs = len(pieces)
    levels, width = pieces[0].shape

    def kernel(*refs):
        refs, out, sem = refs[:xs], refs[xs], refs[xs + 1]
        copies = []
        for k in range(xs):
            x = lax.rem(lax.axis_index("x") + xs - k, xs)
            columns = pl.ds(pl.multiple_of(x * width, width), width)
            copies.append(pltpu.make_async_copy(refs[k], out.at[:, columns], sem.at[k]))
            copies[-1].start()
        for copy in copies:
            copy.wait()

    return pl.pallas_call(
        kernel,
        out_shape=jax.ShapeDtypeStruct((levels, xs * width), jnp.bfloat16),
        in_specs=[VMEM] * xs,
        out_specs=HBM,
        scratch_shapes=[pltpu.SemaphoreType.DMA((xs,))],
        compiler_params=pltpu.CompilerParams(vmem_limit_bytes=8 * 1024 * 1024),
        name="assemble",
    )(*pieces)


def increment(control, corr_offsets, corr_blocks, interp_index, interp_blocks, perturbations):
    members, levels, width = control.shape
    breadth = corr_blocks.shape[2]
    xs = lax.axis_size("x")
    zs = lax.axis_size("z")
    members_all = members * zs * xs
    factor = float(1.0 / (members_all - 1) ** 0.5)
    rows = control.reshape(members * levels, width)
    first, second = tile_halos(rows, HR * breadth)
    smoothed, outer, halo_corr, interp, pert = smooth_own(
        rows, corr_offsets, corr_blocks, interp_blocks,
        perturbations.reshape(members * levels, width),
    )
    pieces = {}
    halo = (outer, halo_corr, first, second)
    for distances in GROUPS:
        results = member_sums(smoothed, interp_index, interp, pert, members, xs, distances, halo)
        if halo:
            smoothed, results, halo = results[0], results[1:], None
        pieces.update(zip(distances, results))

    def along_x(piece, k):
        return lax.ppermute(piece, "x", [(i, (i + k) % xs) for i in range(xs)])

    received = [pieces[0]]
    for k in pieces:
        if k:
            received.append(along_x(pieces[k], k))
    total = sum_pieces(received)
    parts = lax.all_to_all(total.reshape(zs, levels // zs, width // xs), "z", 0, 0)
    column = lax.all_to_all(sum_received(parts, factor), "z", 0, 0)
    column = column.reshape(levels, width // xs)
    return assemble([column] + [along_x(column, k) for k in range(1, xs)])


def solution(mesh):
    zs = 8
    xs = mesh.shape["mem"] // zs
    inner_mesh = jax.sharding.Mesh(
        mesh.devices.reshape(mesh.shape["dom"], zs, xs), ("dom", "z", "x")
    )
    mem = ("z", "x")
    in_specs = (
        P(mem, None, "dom"),
        P("dom", None),
        P("dom", None, None, None),
        P("dom", None),
        P("dom", None, None, None),
        P(mem, None, "dom"),
    )
    out_specs = P(None, "dom")
    return jax.shard_map(
        increment, mesh=inner_mesh, in_specs=in_specs, out_specs=out_specs, check_vma=False
    )
```

```python
import jax
import jax.numpy as jnp
from jax import lax
from jax.experimental import pallas as pl
from jax.experimental.pallas import tpu as pltpu
from jax.sharding import PartitionSpec as P

HR = 2
GROUPS = ((2,), (3,), (1,), (0,))
STAGES = (2, 6)
LATER = 0
K1_LIMIT = 24
K2_LIMIT = 24
HBM = pl.BlockSpec(memory_space=pltpu.HBM)
VMEM = pl.BlockSpec(memory_space=pltpu.VMEM)


def in_hbm(array):
    return pltpu.with_memory_space_constraint(array, pltpu.HBM)


def tile_halos(rows, width):
    span = rows.shape[1] - width

    def kernel(rows_hbm, first, second, sem):
        odd = lax.rem(lax.axis_index("dom"), 2)
        copies = [
            pltpu.make_async_copy(
                rows_hbm.at[:, pl.ds(pl.multiple_of(part * span, width), width)], out, sem.at[i]
            )
            for i, (part, out) in enumerate(((odd, first), (1 - odd, second)))
        ]
        for copy in copies:
            copy.start()
        for copy in copies:
            copy.wait()

    edge = jax.ShapeDtypeStruct((rows.shape[0], width), rows.dtype)
    first, second = pl.pallas_call(
        kernel,
        out_shape=(edge, edge),
        in_specs=[HBM],
        out_specs=(VMEM, VMEM),
        scratch_shapes=[pltpu.SemaphoreType.DMA((2,))],
        compiler_params=pltpu.CompilerParams(vmem_limit_bytes=8 * 1024 * 1024),
        name="tile_edges",
    )(in_hbm(rows))
    count = lax.axis_size("dom")
    above = [(i, (i + 1 if i % 2 else i - 1) % count) for i in range(count)]
    within = [(i, i - 1 if i % 2 else i + 1) for i in range(count)]
    return lax.ppermute(first, "dom", above), lax.ppermute(second, "dom", within)


def smooth_own(control, corr_offsets, corr_blocks, interp_blocks, perturbations):
    rows, width = control.shape
    blocks, stored, breadth = corr_blocks.shape[:3]
    pairs = blocks // 2
    pair = 2 * breadth
    span = 2 + 2 * HR
    halo = HR * breadth

    def kernel(
        offsets_hbm, control_hbm, corr_hbm, interp_hbm, pert_hbm, out, outer, halo_corr, interp,
        pert, offsets, tile, held, corr, offsets_sem, tile_sem, corr_sem, later_sem,
    ):
        def tile_copy(c):
            columns = pl.ds(pl.multiple_of(c * pair, pair), pair)
            return pltpu.make_async_copy(
                control_hbm.at[:, columns], tile.at[:, columns], tile_sem.at[c]
            )

        def stored_copy(c):
            both = pl.ds(2 * c, 2)
            return pltpu.make_async_copy(corr_hbm.at[both], held.at[both], corr_sem.at[c])

        def lay_out(c):
            zero = jnp.zeros((breadth, breadth), corr.dtype)
            for j in range(2):
                columns = pl.ds(j * breadth, breadth)
                absent = HR + j
                for s in range(stored):
                    offset = offsets[s, 2 * c + j]
                    absent = absent - offset
                    row = pl.multiple_of((offset + HR + j) * breadth, breadth)
                    corr[c, pl.ds(row, breadth), columns] = held[2 * c + j, s]
                corr[c, pl.ds(pl.multiple_of(absent * breadth, breadth), breadth), columns] = zero
                far = (1 - j) * (span - 1)
                corr[c, far * breadth : (far + 1) * breadth, columns] = zero

        def later_copies(g):
            share = rows // len(stages)
            some = pl.ds(g * share, share)
            count = interp_hbm.shape[0] // len(stages)
            blocks_of = pl.ds(g * count, count)
            return (
                pltpu.make_async_copy(pert_hbm.at[some], pert.at[some], later_sem.at[g, 0]),
                pltpu.make_async_copy(
                    interp_hbm.at[blocks_of], interp.at[blocks_of], later_sem.at[g, 1]
                ),
            )

        stages = [range(sum(STAGES[:g]), sum(STAGES[: g + 1])) for g in range(len(STAGES))]
        offsets_copy = pltpu.make_async_copy(offsets_hbm, offsets, offsets_sem)
        offsets_copy.start()
        tile_ends = [min(stage[-1] + 2, pairs) for stage in stages]
        for g, stage in enumerate(stages):

            @pl.loop(tile_ends[g - 1] if g else 0, tile_ends[g])
            def _(c):
                tile_copy(c).start()

            @pl.loop(stage[0], stage[-1] + 1)
            def _(c):
                stored_copy(c).start()

        for g, stage in enumerate(stages):
            for c in stage:
                stored_copy(c).wait()
            if g == 0:
                offsets_copy.wait()
            for c in stage:
                lay_out(c)
            for c in range(tile_ends[g - 1] if g else 0, tile_ends[g]):
                tile_copy(c).wait()
            if g == LATER:
                for h in range(len(stages)):
                    for copy in later_copies(h):
                        copy.start()
            for c in stage:
                first = max(2 * c - HR, 0)
                last = min(2 * c + 2 + HR, blocks)
                start = (first - (2 * c - HR)) * breadth
                depth = (last - first) * breadth
                result = jnp.dot(
                    tile[:, first * breadth : last * breadth],
                    corr[c, start : start + depth, :],
                    preferred_element_type=jnp.float32,
                )
                if c == 0 or c == pairs - 1:
                    side = min(c, 1)
                    outer[side] = result
                    low = side * (span * breadth - halo)
                    halo_corr[side] = corr[c, low : low + halo, :]
                else:
                    result = result.astype(jnp.bfloat16)
                    out[2 * c] = result[:, :breadth]
                    out[2 * c + 1] = result[:, breadth:]
        for g in range(len(stages)):
            for copy in later_copies(g):
                copy.wait()

    return pl.pallas_call(
        kernel,
        out_shape=(
            jax.ShapeDtypeStruct((blocks, rows, breadth), jnp.bfloat16),
            jax.ShapeDtypeStruct((2, rows, pair), jnp.float32),
            jax.ShapeDtypeStruct((2, halo, pair), jnp.bfloat16),
            jax.ShapeDtypeStruct(interp_blocks.shape, jnp.bfloat16),
            jax.ShapeDtypeStruct(perturbations.shape, jnp.bfloat16),
        ),
        in_specs=[HBM] * 5,
        out_specs=(VMEM,) * 5,
        scratch_shapes=[
            pltpu.SMEM((stored, blocks), jnp.int32),
            pltpu.VMEM((rows, width), jnp.bfloat16),
            pltpu.VMEM(corr_blocks.shape, jnp.bfloat16),
            pltpu.VMEM((pairs, span * breadth, pair), jnp.bfloat16),
            pltpu.SemaphoreType.DMA,
            pltpu.SemaphoreType.DMA((pairs,)),
            pltpu.SemaphoreType.DMA((pairs,)),
            pltpu.SemaphoreType.DMA((len(STAGES), 2)),
        ],
        compiler_params=pltpu.CompilerParams(vmem_limit_bytes=K1_LIMIT * 1024 * 1024),
        cost_estimate=pl.CostEstimate(
            flops=2 * rows * stored * breadth * breadth * blocks,
            bytes_accessed=4 * rows * width,
            transcendentals=0,
        ),
        name="smooth_own",
    )(
        in_hbm(corr_offsets.T), in_hbm(control), in_hbm(corr_blocks), in_hbm(interp_blocks),
        in_hbm(perturbations),
    )


def member_sums(smoothed, interp_index, interp_blocks, perturbations, members, xs, distances, halo=None):
    blocks, rows, breadth = smoothed.shape
    column_blocks, feeding = interp_blocks.shape[:2]
    levels = rows // members
    share = column_blocks // xs

    def kernel(index, interp, pert, *refs):
        outs = refs[-len(distances) :]
        position = lax.axis_index("x")
        if halo is None:
            smooth = refs[0]
        else:
            outer_ref, corr, first_ref, second_ref, smooth = refs[1:6]
            odd = lax.rem(lax.axis_index("dom"), 2)
            for side, halo_ref in ((1 - odd, second_ref), (odd, first_ref)):
                result = outer_ref[side] + jnp.dot(
                    halo_ref[...], corr[side], preferred_element_type=jnp.float32
                )
                result = result.astype(jnp.bfloat16)
                b = side * (blocks - HR)
                smooth[b] = result[:, :breadth]
                smooth[b + 1] = result[:, breadth:]
        for distance, out in zip(distances, outs):
            piece = lax.rem(position + distance, xs)
            for i in range(share):
                q = piece * share + i
                lhs = jnp.concatenate([smooth[index[q, k]] for k in range(feeding)], axis=1)
                spread = jnp.dot(
                    lhs,
                    interp[q].reshape(feeding * breadth, breadth),
                    preferred_element_type=jnp.float32,
                )
                columns = pl.ds(pl.multiple_of(q * breadth, breadth), breadth)
                term = pert[:, columns].astype(jnp.float32) * spread
                total = jnp.sum(term.reshape(members, levels, breadth), axis=0)
                out[:, i * breadth : (i + 1) * breadth] = total.astype(jnp.bfloat16)

    pieces = tuple(
        jax.ShapeDtypeStruct((levels, share * breadth), jnp.bfloat16) for _ in distances
    )
    operands = (interp_blocks, perturbations, smoothed) + (halo or ())
    return pl.pallas_call(
        kernel,
        out_shape=pieces if halo is None else (smoothed,) + pieces,
        in_specs=[VMEM] * (1 + len(operands)),
        out_specs=(VMEM,) * (len(pieces) + (halo is not None)),
        input_output_aliases={} if halo is None else {3: 0},
        compiler_params=pltpu.CompilerParams(vmem_limit_bytes=K2_LIMIT * 1024 * 1024),
        cost_estimate=pl.CostEstimate(
            flops=2 * rows * feeding * breadth * breadth * (share * len(distances) + 1),
            bytes_accessed=6 * rows * share * breadth * len(distances),
            transcendentals=0,
        ),
        name="member_sums",
    )(interp_index, *operands)


def sum_pieces(pieces):
    def kernel(*refs):
        total = refs[0][...].astype(jnp.float32)
        for ref in refs[1:-1]:
            total = total + ref[...].astype(jnp.float32)
        refs[-1][...] = total.astype(jnp.bfloat16)

    return pl.pallas_call(
        kernel,
        out_shape=jax.ShapeDtypeStruct(pieces[0].shape, jnp.bfloat16),
        in_specs=[VMEM] * len(pieces),
        out_specs=VMEM,
        compiler_params=pltpu.CompilerParams(vmem_limit_bytes=8 * 1024 * 1024),
        name="sum_pieces",
    )(*pieces)


def sum_received(parts, factor):
    def kernel(parts_ref, out_ref):
        total = jnp.sum(parts_ref[...].astype(jnp.float32), axis=0) * factor
        out_ref[...] = jnp.broadcast_to(total.astype(jnp.bfloat16)[None], out_ref.shape)

    return pl.pallas_call(
        kernel,
        out_shape=jax.ShapeDtypeStruct(parts.shape, jnp.bfloat16),
        in_specs=[VMEM],
        out_specs=VMEM,
        compiler_params=pltpu.CompilerParams(vmem_limit_bytes=8 * 1024 * 1024),
        name="sum_received",
    )(parts)


def assemble(pieces):
    xs = len(pieces)
    levels, width = pieces[0].shape

    def kernel(*refs):
        refs, out, sem = refs[:xs], refs[xs], refs[xs + 1]
        copies = []
        for k in range(xs):
            x = lax.rem(lax.axis_index("x") + xs - k, xs)
            columns = pl.ds(pl.multiple_of(x * width, width), width)
            copies.append(pltpu.make_async_copy(refs[k], out.at[:, columns], sem.at[k]))
            copies[-1].start()
        for copy in copies:
            copy.wait()

    return pl.pallas_call(
        kernel,
        out_shape=jax.ShapeDtypeStruct((levels, xs * width), jnp.bfloat16),
        in_specs=[VMEM] * xs,
        out_specs=HBM,
        scratch_shapes=[pltpu.SemaphoreType.DMA((xs,))],
        compiler_params=pltpu.CompilerParams(vmem_limit_bytes=8 * 1024 * 1024),
        name="assemble",
    )(*pieces)


def increment(control, corr_offsets, corr_blocks, interp_index, interp_blocks, perturbations):
    members, levels, width = control.shape
    breadth = corr_blocks.shape[2]
    xs = lax.axis_size("x")
    zs = lax.axis_size("z")
    members_all = members * zs * xs
    factor = float(1.0 / (members_all - 1) ** 0.5)
    rows = control.reshape(members * levels, width)
    first, second = tile_halos(rows, HR * breadth)
    smoothed, outer, halo_corr, interp, pert = smooth_own(
        rows, corr_offsets, corr_blocks, interp_blocks,
        perturbations.reshape(members * levels, width),
    )
    pieces = {}
    halo = (outer, halo_corr, first, second)
    for distances in GROUPS:
        results = member_sums(smoothed, interp_index, interp, pert, members, xs, distances, halo)
        if halo:
            smoothed, results, halo = results[0], results[1:], None
        pieces.update(zip(distances, results))

    def along_x(piece, k):
        return lax.ppermute(piece, "x", [(i, (i + k) % xs) for i in range(xs)])

    received = [pieces[0]]
    for k in pieces:
        if k:
            received.append(along_x(pieces[k], k))
    total = sum_pieces(received)
    parts = lax.all_to_all(total.reshape(zs, levels // zs, width // xs), "z", 0, 0)
    column = lax.all_to_all(sum_received(parts, factor), "z", 0, 0)
    column = column.reshape(levels, width // xs)
    return assemble([column] + [along_x(column, k) for k in range(1, xs)])


def solution(mesh):
    zs = 8
    xs = mesh.shape["mem"] // zs
    inner_mesh = jax.sharding.Mesh(
        mesh.devices.reshape(mesh.shape["dom"], zs, xs), ("dom", "z", "x")
    )
    mem = ("z", "x")
    in_specs = (
        P(mem, None, "dom"),
        P("dom", None),
        P("dom", None, None, None),
        P("dom", None),
        P("dom", None, None, None),
        P(mem, None, "dom"),
    )
    out_specs = P(None, "dom")
    return jax.shard_map(
        increment, mesh=inner_mesh, in_specs=in_specs, out_specs=out_specs, check_vma=False
    )
```

```python
import jax
import jax.numpy as jnp
from jax import lax
from jax.experimental import pallas as pl
from jax.experimental.pallas import tpu as pltpu
from jax.sharding import PartitionSpec as P

HR = 2
GROUPS = ((2,), (3, 1), (0,))
BACK = (2, 1, 3)
STAGES = (2, 6)
LATER = 0
K1_LIMIT = 24
K2_LIMIT = 24
HBM = pl.BlockSpec(memory_space=pltpu.HBM)
VMEM = pl.BlockSpec(memory_space=pltpu.VMEM)


def in_hbm(array):
    return pltpu.with_memory_space_constraint(array, pltpu.HBM)


def tile_halos(rows, width):
    span = rows.shape[1] - width

    def kernel(rows_hbm, first, second, sem):
        odd = lax.rem(lax.axis_index("dom"), 2)
        copies = [
            pltpu.make_async_copy(
                rows_hbm.at[:, pl.ds(pl.multiple_of(part * span, width), width)], out, sem.at[i]
            )
            for i, (part, out) in enumerate(((odd, first), (1 - odd, second)))
        ]
        for copy in copies:
            copy.start()
        for copy in copies:
            copy.wait()

    edge = jax.ShapeDtypeStruct((rows.shape[0], width), rows.dtype)
    first, second = pl.pallas_call(
        kernel,
        out_shape=(edge, edge),
        in_specs=[HBM],
        out_specs=(VMEM, VMEM),
        scratch_shapes=[pltpu.SemaphoreType.DMA((2,))],
        compiler_params=pltpu.CompilerParams(vmem_limit_bytes=8 * 1024 * 1024),
        name="tile_edges",
    )(in_hbm(rows))
    count = lax.axis_size("dom")
    above = [(i, (i + 1 if i % 2 else i - 1) % count) for i in range(count)]
    within = [(i, i - 1 if i % 2 else i + 1) for i in range(count)]
    return lax.ppermute(first, "dom", above), lax.ppermute(second, "dom", within)


def smooth_own(control, corr_offsets, corr_blocks, interp_blocks, perturbations):
    rows, width = control.shape
    blocks, stored, breadth = corr_blocks.shape[:3]
    pairs = blocks // 2
    pair = 2 * breadth
    span = 2 + 2 * HR
    halo = HR * breadth

    def kernel(
        offsets_hbm, control_hbm, corr_hbm, interp_hbm, pert_hbm, out, outer, halo_corr, interp,
        pert, offsets, tile, held, corr, offsets_sem, tile_sem, corr_sem, later_sem,
    ):
        def tile_copy(c):
            columns = pl.ds(pl.multiple_of(c * pair, pair), pair)
            return pltpu.make_async_copy(
                control_hbm.at[:, columns], tile.at[:, columns], tile_sem.at[c]
            )

        def stored_copy(c):
            both = pl.ds(2 * c, 2)
            return pltpu.make_async_copy(corr_hbm.at[both], held.at[both], corr_sem.at[c])

        def lay_out(c):
            zero = jnp.zeros((breadth, breadth), corr.dtype)
            for j in range(2):
                columns = pl.ds(j * breadth, breadth)
                absent = HR + j
                for s in range(stored):
                    offset = offsets[s, 2 * c + j]
                    absent = absent - offset
                    row = pl.multiple_of((offset + HR + j) * breadth, breadth)
                    corr[c, pl.ds(row, breadth), columns] = held[2 * c + j, s]
                corr[c, pl.ds(pl.multiple_of(absent * breadth, breadth), breadth), columns] = zero
                far = (1 - j) * (span - 1)
                corr[c, far * breadth : (far + 1) * breadth, columns] = zero

        def later_copies(g):
            share = rows // len(stages)
            some = pl.ds(g * share, share)
            count = interp_hbm.shape[0] // len(stages)
            blocks_of = pl.ds(g * count, count)
            return (
                pltpu.make_async_copy(pert_hbm.at[some], pert.at[some], later_sem.at[g, 0]),
                pltpu.make_async_copy(
                    interp_hbm.at[blocks_of], interp.at[blocks_of], later_sem.at[g, 1]
                ),
            )

        stages = [range(sum(STAGES[:g]), sum(STAGES[: g + 1])) for g in range(len(STAGES))]
        offsets_copy = pltpu.make_async_copy(offsets_hbm, offsets, offsets_sem)
        offsets_copy.start()
        tile_ends = [min(stage[-1] + 2, pairs) for stage in stages]
        for g, stage in enumerate(stages):

            @pl.loop(tile_ends[g - 1] if g else 0, tile_ends[g])
            def _(c):
                tile_copy(c).start()

            @pl.loop(stage[0], stage[-1] + 1)
            def _(c):
                stored_copy(c).start()

        for g, stage in enumerate(stages):
            for c in stage:
                stored_copy(c).wait()
            if g == 0:
                offsets_copy.wait()
            for c in stage:
                lay_out(c)
            for c in range(tile_ends[g - 1] if g else 0, tile_ends[g]):
                tile_copy(c).wait()
            if g == LATER:
                for h in range(len(stages)):
                    for copy in later_copies(h):
                        copy.start()
            for c in stage:
                first = max(2 * c - HR, 0)
                last = min(2 * c + 2 + HR, blocks)
                start = (first - (2 * c - HR)) * breadth
                depth = (last - first) * breadth
                result = jnp.dot(
                    tile[:, first * breadth : last * breadth],
                    corr[c, start : start + depth, :],
                    preferred_element_type=jnp.float32,
                )
                if c == 0 or c == pairs - 1:
                    side = min(c, 1)
                    outer[side] = result
                    low = side * (span * breadth - halo)
                    halo_corr[side] = corr[c, low : low + halo, :]
                else:
                    result = result.astype(jnp.bfloat16)
                    out[2 * c] = result[:, :breadth]
                    out[2 * c + 1] = result[:, breadth:]
        for g in range(len(stages)):
            for copy in later_copies(g):
                copy.wait()

    return pl.pallas_call(
        kernel,
        out_shape=(
            jax.ShapeDtypeStruct((blocks, rows, breadth), jnp.bfloat16),
            jax.ShapeDtypeStruct((2, rows, pair), jnp.float32),
            jax.ShapeDtypeStruct((2, halo, pair), jnp.bfloat16),
            jax.ShapeDtypeStruct(interp_blocks.shape, jnp.bfloat16),
            jax.ShapeDtypeStruct(perturbations.shape, jnp.bfloat16),
        ),
        in_specs=[HBM] * 5,
        out_specs=(VMEM,) * 5,
        scratch_shapes=[
            pltpu.SMEM((stored, blocks), jnp.int32),
            pltpu.VMEM((rows, width), jnp.bfloat16),
            pltpu.VMEM(corr_blocks.shape, jnp.bfloat16),
            pltpu.VMEM((pairs, span * breadth, pair), jnp.bfloat16),
            pltpu.SemaphoreType.DMA,
            pltpu.SemaphoreType.DMA((pairs,)),
            pltpu.SemaphoreType.DMA((pairs,)),
            pltpu.SemaphoreType.DMA((len(STAGES), 2)),
        ],
        compiler_params=pltpu.CompilerParams(vmem_limit_bytes=K1_LIMIT * 1024 * 1024),
        cost_estimate=pl.CostEstimate(
            flops=2 * rows * stored * breadth * breadth * blocks,
            bytes_accessed=4 * rows * width,
            transcendentals=0,
        ),
        name="smooth_own",
    )(
        in_hbm(corr_offsets.T), in_hbm(control), in_hbm(corr_blocks), in_hbm(interp_blocks),
        in_hbm(perturbations),
    )


def member_sums(smoothed, interp_index, interp_blocks, perturbations, members, xs, distances, halo=None):
    blocks, rows, breadth = smoothed.shape
    column_blocks, feeding = interp_blocks.shape[:2]
    levels = rows // members
    share = column_blocks // xs

    def kernel(index, interp, pert, *refs):
        outs = refs[-len(distances) :]
        position = lax.axis_index("x")
        if halo is None:
            smooth = refs[0]
        else:
            outer_ref, corr, first_ref, second_ref, smooth = refs[1:6]
            odd = lax.rem(lax.axis_index("dom"), 2)
            for side, halo_ref in ((1 - odd, second_ref), (odd, first_ref)):
                result = outer_ref[side] + jnp.dot(
                    halo_ref[...], corr[side], preferred_element_type=jnp.float32
                )
                result = result.astype(jnp.bfloat16)
                b = side * (blocks - HR)
                smooth[b] = result[:, :breadth]
                smooth[b + 1] = result[:, breadth:]
        for distance, out in zip(distances, outs):
            piece = lax.rem(position + distance, xs)
            for i in range(share):
                q = piece * share + i
                lhs = jnp.concatenate([smooth[index[q, k]] for k in range(feeding)], axis=1)
                spread = jnp.dot(
                    lhs,
                    interp[q].reshape(feeding * breadth, breadth),
                    preferred_element_type=jnp.float32,
                )
                columns = pl.ds(pl.multiple_of(q * breadth, breadth), breadth)
                term = pert[:, columns].astype(jnp.float32) * spread
                total = jnp.sum(term.reshape(members, levels, breadth), axis=0)
                out[:, i * breadth : (i + 1) * breadth] = total.astype(jnp.bfloat16)

    pieces = tuple(
        jax.ShapeDtypeStruct((levels, share * breadth), jnp.bfloat16) for _ in distances
    )
    operands = (interp_blocks, perturbations, smoothed) + (halo or ())
    return pl.pallas_call(
        kernel,
        out_shape=pieces if halo is None else (smoothed,) + pieces,
        in_specs=[VMEM] * (1 + len(operands)),
        out_specs=(VMEM,) * (len(pieces) + (halo is not None)),
        input_output_aliases={} if halo is None else {3: 0},
        compiler_params=pltpu.CompilerParams(vmem_limit_bytes=K2_LIMIT * 1024 * 1024),
        cost_estimate=pl.CostEstimate(
            flops=2 * rows * feeding * breadth * breadth * (share * len(distances) + 1),
            bytes_accessed=6 * rows * share * breadth * len(distances),
            transcendentals=0,
        ),
        name="member_sums",
    )(interp_index, *operands)


def sum_pieces(pieces):
    def kernel(*refs):
        total = refs[0][...].astype(jnp.float32)
        for ref in refs[1:-1]:
            total = total + ref[...].astype(jnp.float32)
        refs[-1][...] = total.astype(jnp.bfloat16)

    return pl.pallas_call(
        kernel,
        out_shape=jax.ShapeDtypeStruct(pieces[0].shape, jnp.bfloat16),
        in_specs=[VMEM] * len(pieces),
        out_specs=VMEM,
        compiler_params=pltpu.CompilerParams(vmem_limit_bytes=8 * 1024 * 1024),
        name="sum_pieces",
    )(*pieces)


def sum_received(parts, factor):
    def kernel(parts_ref, out_ref):
        total = jnp.sum(parts_ref[...].astype(jnp.float32), axis=0) * factor
        out_ref[...] = jnp.broadcast_to(total.astype(jnp.bfloat16)[None], out_ref.shape)

    return pl.pallas_call(
        kernel,
        out_shape=jax.ShapeDtypeStruct(parts.shape, jnp.bfloat16),
        in_specs=[VMEM],
        out_specs=VMEM,
        compiler_params=pltpu.CompilerParams(vmem_limit_bytes=8 * 1024 * 1024),
        name="sum_received",
    )(parts)


def assemble(pieces):
    xs = len(pieces)
    levels, width = pieces[0].shape

    def kernel(*refs):
        refs, out, sem = refs[:xs], refs[xs], refs[xs + 1]
        copies = []
        for k in range(xs):
            x = lax.rem(lax.axis_index("x") + xs - k, xs)
            columns = pl.ds(pl.multiple_of(x * width, width), width)
            copies.append(pltpu.make_async_copy(refs[k], out.at[:, columns], sem.at[k]))
            copies[-1].start()
        for copy in copies:
            copy.wait()

    return pl.pallas_call(
        kernel,
        out_shape=jax.ShapeDtypeStruct((levels, xs * width), jnp.bfloat16),
        in_specs=[VMEM] * xs,
        out_specs=HBM,
        scratch_shapes=[pltpu.SemaphoreType.DMA((xs,))],
        compiler_params=pltpu.CompilerParams(vmem_limit_bytes=8 * 1024 * 1024),
        name="assemble",
    )(*pieces)


def increment(control, corr_offsets, corr_blocks, interp_index, interp_blocks, perturbations):
    members, levels, width = control.shape
    breadth = corr_blocks.shape[2]
    xs = lax.axis_size("x")
    zs = lax.axis_size("z")
    members_all = members * zs * xs
    factor = float(1.0 / (members_all - 1) ** 0.5)
    rows = control.reshape(members * levels, width)
    first, second = tile_halos(rows, HR * breadth)
    smoothed, outer, halo_corr, interp, pert = smooth_own(
        rows, corr_offsets, corr_blocks, interp_blocks,
        perturbations.reshape(members * levels, width),
    )
    pieces = {}
    halo = (outer, halo_corr, first, second)
    for distances in GROUPS:
        results = member_sums(smoothed, interp_index, interp, pert, members, xs, distances, halo)
        if halo:
            smoothed, results, halo = results[0], results[1:], None
        pieces.update(zip(distances, results))

    def along_x(piece, k):
        return lax.ppermute(piece, "x", [(i, (i + k) % xs) for i in range(xs)])

    received = [pieces[0]]
    for k in pieces:
        if k:
            received.append(along_x(pieces[k], k))
    total = sum_pieces(received)
    parts = lax.all_to_all(total.reshape(zs, levels // zs, width // xs), "z", 0, 0)
    column = lax.all_to_all(sum_received(parts, factor), "z", 0, 0)
    column = column.reshape(levels, width // xs)
    others = {}
    for k in BACK:
        others[k] = along_x(column, k)
    return assemble([column] + [others[k] for k in range(1, xs)])


def solution(mesh):
    zs = 8
    xs = mesh.shape["mem"] // zs
    inner_mesh = jax.sharding.Mesh(
        mesh.devices.reshape(mesh.shape["dom"], zs, xs), ("dom", "z", "x")
    )
    mem = ("z", "x")
    in_specs = (
        P(mem, None, "dom"),
        P("dom", None),
        P("dom", None, None, None),
        P("dom", None),
        P("dom", None, None, None),
        P(mem, None, "dom"),
    )
    out_specs = P(None, "dom")
    return jax.shard_map(
        increment, mesh=inner_mesh, in_specs=in_specs, out_specs=out_specs, check_vma=False
    )
```
